32 devices in a mesh: dp: 8 (over z, y), tp: 4 (over x, core).
Axes of the slice: x: 2, y: 2, z: 4, core: 2. Of those that a mesh axis runs over, the one named last changes fastest.
Arguments:
- partial_up: bfloat16 [8, 1024, 4096], P('dp', None, 'tp'), may hold values from -4 to 4
- partial_down: bfloat16 [8, 4096, 1024], P('dp', 'tp'), may hold values from -4 to 4
- partial_norm: bfloat16 [8, 1024], P('dp'), may hold values from -8 to 8
- master_up: float32 [1024, 4096], P('dp', 'tp'), may hold values from -0.25 to 0.25
- master_down: float32 [4096, 1024], P('tp', 'dp'), may hold values from -0.125 to 0.125
- master_norm: float32 [1024], P('dp'), may hold values from 0.25 to 1.75
- memory_up: float32 [1024, 4096], P('dp', 'tp'), may hold values from 0.0001953125 to 0.001953125
- memory_down: float32 [4096, 1024], P('tp', 'dp'), may hold values from 4.8828126e-05 to 0.00048828125
- memory_norm: float32 [1024], P('dp'), may hold values from 0.05 to 0.8
Outputs:
- compute_up: bfloat16 [1024, 4096], P(None, 'tp')
- compute_down: bfloat16 [4096, 1024], P('tp')
- compute_norm: bfloat16 [1024], replicated
- stepped_up: float32 [1024, 4096], P('dp', 'tp')
- stepped_down: float32 [4096, 1024], P('tp', 'dp')
- stepped_norm: float32 [1024], P('dp')
- state_new_up: float32 [1024, 4096], P('dp', 'tp')
- state_new_down: float32 [4096, 1024], P('tp', 'dp')
- state_new_norm: float32 [1024], P('dp')
The draws below stay inside these ranges and needn't reach their ends.
All inputs are finite; a program needn't handle non-finite values.
Results may differ from the reference program's by a relative error of at most 0.001.
Values may be sent and summed in bfloat16 or wider, within the bound.
A program may use at most 64 MiB of HBM per device.

```python
import jax
import jax.numpy as jnp
from jax import lax

WIDTH = 1024
INNER = 4096
REPLICAS = 8


def raised(values, own_key, source, target, shards_of, factor):
    def block_of(axis_at):
        return (jnp.arange(values.shape[axis_at]) // (values.shape[axis_at] // shards_of)).reshape((-1,) + (1,) * (values.ndim - 1 - axis_at))

    near = jax.random.permutation(own_key, shards_of)[block_of(target)]
    far = (block_of(target) + shards_of // 2) % shards_of
    return jnp.where((block_of(source) == near) | (block_of(source) == far), factor * values, values)


def block_levels(rng, extent, cuts, low, largest):
    def one(dim, shards_of):
        steps = jax.random.uniform(jax.random.fold_in(jax.random.fold_in(rng, 6), dim), (shards_of,), jnp.float32, low / len(cuts), largest / len(cuts))
        return jnp.repeat(jnp.exp(steps), extent[dim] // shards_of).reshape((-1,) + (1,) * (len(extent) - dim - 1))

    factor_of = one(*cuts[0])
    for cut in cuts[1:]:
        factor_of = factor_of * one(*cut)
    return factor_of


def noise_with(key, extent, width, limit, shards, heavy, kind=jnp.bfloat16):
    array = width * jax.random.normal(key, extent, jnp.float32)
    if shards:
        array = array * block_levels(key, extent, shards, -0.22, 0.18)
    return jnp.clip(raised(array, jax.random.fold_in(key, 3), *heavy), -limit, limit).astype(kind)


def setup_inputs(seed: int = 0) -> dict:
    streams_of = jax.random.split(jax.random.key(seed), 10)
    partial_up = noise_with(streams_of[0], (REPLICAS, WIDTH, INNER), 0.5, 4.0, ((0, 8), (2, 4)), (0, 1, 8, 2.0))
    partial_down = noise_with(streams_of[1], (REPLICAS, INNER, WIDTH), 0.5, 4.0, ((0, 8), (1, 4)), (0, 2, 8, 2.0))
    partial_norm = noise_with(streams_of[2], (REPLICAS, WIDTH), 1.0, 8.0, ((0, 8),), (0, 1, 8, 2.0))
    master_up = noise_with(streams_of[3], (WIDTH, INNER), WIDTH ** -0.5, 0.25, ((0, 8), (1, 4)), (1, 0, 8, 2.0), jnp.float32)
    master_down = noise_with(streams_of[4], (INNER, WIDTH), INNER ** -0.5, 0.125, ((0, 4), (1, 8)), (0, 1, 8, 2.0), jnp.float32)
    master_norm = jnp.clip(1.0 + 0.15 * jax.random.normal(streams_of[5], (WIDTH,), jnp.float32), 0.25, 1.75)
    memory_up = jnp.clip(0.0001953125 + 0.0017578125 * jax.random.uniform(streams_of[6], (WIDTH, INNER), jnp.float32) ** block_levels(streams_of[6], (WIDTH, INNER), ((0, 8), (1, 4)), -0.2, 0.2), 0.0001953125, 0.001953125)
    memory_down = jnp.clip(4.882812572759576e-05 + 0.0004394531 * jax.random.uniform(streams_of[7], (INNER, WIDTH), jnp.float32) ** block_levels(streams_of[7], (INNER, WIDTH), ((0, 4), (1, 8)), -0.2, 0.2), 4.882812572759576e-05, 0.00048828125)
    memory_norm = jnp.clip(0.05 + 0.75 * jax.random.uniform(streams_of[8], (WIDTH,), jnp.float32) ** block_levels(streams_of[8], (WIDTH,), ((0, 8),), -0.2, 0.2), 0.05, 0.8)
    return {"partial_up": partial_up, "partial_down": partial_down, "partial_norm": partial_norm, "master_up": master_up, "master_down": master_down, "master_norm": master_norm, "memory_up": memory_up, "memory_down": memory_down, "memory_norm": memory_norm}


learn_rate = 0.025
hold_rate = 0.8

def reference(partial_up, partial_down, partial_norm, master_up, master_down, master_norm, memory_up, memory_down, memory_norm):
    mean_up = lax.optimization_barrier(jnp.sum(partial_up.astype(jnp.float32), axis=0)) * REPLICAS ** (-0.5)
    mean_down = lax.optimization_barrier(jnp.sum(partial_down.astype(jnp.float32), axis=0)) * REPLICAS ** (-0.5)
    mean_norm = lax.optimization_barrier(jnp.sum(partial_norm.astype(jnp.float32), axis=0)) * REPLICAS ** (-0.5)
    ratio_up = jnp.sqrt(lax.optimization_barrier(jnp.sum(master_up * master_up, axis=1, keepdims=True))) * lax.rsqrt(lax.optimization_barrier(jnp.sum(mean_up * mean_up, axis=1, keepdims=True)) + 1e-06)
    mean_up = mean_up * ratio_up
    ratio_down = jnp.sqrt(lax.optimization_barrier(jnp.sum(master_down * master_down, axis=0, keepdims=True))) * lax.rsqrt(lax.optimization_barrier(jnp.sum(mean_down * mean_down, axis=0, keepdims=True)) + 1e-06)
    mean_down = mean_down * ratio_down
    state_new_up = hold_rate * memory_up + (1.0 - hold_rate) * mean_up * mean_up
    stepped_up = master_up - learn_rate * mean_up * lax.rsqrt(state_new_up + 1e-06)
    state_new_down = hold_rate * memory_down + (1.0 - hold_rate) * mean_down * mean_down
    stepped_down = master_down - learn_rate * mean_down * lax.rsqrt(state_new_down + 1e-06)
    state_new_norm = hold_rate * memory_norm + (1.0 - hold_rate) * mean_norm * mean_norm
    stepped_norm = master_norm - learn_rate * mean_norm * lax.rsqrt(state_new_norm + 1e-06)
    compute_up = stepped_up.astype(jnp.bfloat16)
    compute_down = stepped_down.astype(jnp.bfloat16)
    compute_norm = stepped_norm.astype(jnp.bfloat16)
    return (compute_up, compute_down, compute_norm, stepped_up, stepped_down, stepped_norm, state_new_up, state_new_down, state_new_norm)
```

```python
import functools

import jax
import jax.numpy as jnp
from jax import lax
from jax.experimental import pallas as pl
from jax.experimental.pallas import tpu as pltpu
from jax.sharding import PartitionSpec as P

learn_rate = 0.025
hold_rate = 0.8
f32 = jnp.float32
bf16 = jnp.bfloat16
MESH = pl.DeviceIdType.MESH


def kernel(
    n, T, Y, K,
    pd, pu, pn, md, ed, mu, eu,
    cd, cu, cn, sd, su, sn, td, tu, tn,
    rd, ru, rn, totd, totu, nsend, nrecv,
    loc, nms, nmr, rss, rsr, nxs, nxr, azs, azr, ays, ayr,
):
    Z = n // Y
    me = lax.axis_index("dp")
    tp = lax.axis_index("tp")
    z, y = me // Y, me % Y
    W = rd.shape[2]
    R = ru.shape[1]
    H = rd.shape[1]
    rc = R // K
    rate = n ** -0.5

    def remote(src, dst, s, r, dev):
        return pltpu.make_async_remote_copy(
            src_ref=src, dst_ref=dst, send_sem=s, recv_sem=r, device_id=dev, device_id_type=MESH
        )

    def up(a, m):
        return pl.multiple_of(a, m)

    peers = [lax.rem(me + o, n) for o in range(1, n)]
    tpeers = [lax.rem(tp + o, T) for o in range(1, T)]

    def src_of(c, d):
        if c == 0:
            return pd.at[0, :, pl.ds(up(d * W, 128), W)]
        return pu.at[0, pl.ds(up(d * R + (c - 1) * rc, 16), rc), :]

    def slot_of(c, s):
        if c == 0:
            return rd.at[s]
        return ru.at[s, pl.ds((c - 1) * rc, rc), :]

    def block_of(c, d):
        if c == 0:
            return cd.at[:, pl.ds(up(d * W, 128), W)]
        return cu.at[pl.ds(up(d * R + (c - 1) * rc, 16), rc), :]

    def local_copy(c):
        return pltpu.make_async_copy(src_of(c, me), slot_of(c, me), loc.at[c])

    def rs_copy(c, o, d):
        return remote(src_of(c, d), slot_of(c, me), rss.at[c, o], rsr.at[c, me], (d, tp))

    def rs_start(c):
        for o, d in enumerate(peers):
            rs_copy(c, o, d).start()

    def rs_wait(c):
        local_copy(c).wait()
        for s in peers:
            remote(slot_of(c, s), slot_of(c, s), rss.at[c, 0], rsr.at[c, s], (s, tp)).wait_recv()

    def nx_copy(c, o, t):
        return remote(nsend.at[c], nrecv.at[c, tp], nxs.at[c, o], nxr.at[c, tp], (me, t))

    def exchange(c, value):
        nsend[c] = value
        nrecv[c, tp] = value
        for o, t in enumerate(tpeers):
            nx_copy(c, o, t).start()
        for t in tpeers:
            remote(nsend.at[c], nrecv.at[c, t], nxs.at[c, 0], nxr.at[c, t], (me, t)).wait_recv()
        total = nrecv[c, 0]
        for t in range(1, T):
            total = total + nrecv[c, t]
        return total

    def update(m, master, memory):
        state = hold_rate * memory + (1.0 - hold_rate) * m * m
        return state, master - learn_rate * m * lax.rsqrt(state + 1e-06)

    def down():
        c, hb = 0, 128
        def add(i, carry):
            rows = pl.ds(up(i * hb, hb), hb)
            acc = rd[0, rows, :].astype(f32)
            for s in range(1, n):
                acc = acc + rd[s, rows, :].astype(f32)
            acc = acc * rate
            totd[rows, :] = acc
            w = md[rows, :]
            return (
                carry[0] + jnp.sum((w * w).reshape(hb // 8, 8, W), axis=0),
                carry[1] + jnp.sum((acc * acc).reshape(hb // 8, 8, W), axis=0),
            )
        zero = jnp.zeros((8, W), f32)
        own, slope = lax.fori_loop(0, H // hb, add, (zero, zero))
        own = jnp.sum(own, axis=0, keepdims=True)
        slope = jnp.sum(slope, axis=0, keepdims=True)
        line = lax.broadcasted_iota(jnp.int32, (8, W), 0)
        total = exchange(c, jnp.where(line == 0, own, slope))
        scale = jnp.sqrt(total[0:1, :]) * lax.rsqrt(total[1:2, :] + 1e-06)
        def step(i, carry):
            rows = pl.ds(up(i * hb, hb), hb)
            state, stepped = update(totd[rows, :] * scale, md[rows, :], ed[rows, :])
            td[rows, :] = state
            sd[rows, :] = stepped
            cd[rows, pl.ds(up(me * W, 128), W)] = stepped.astype(bf16)
            return carry
        lax.fori_loop(0, H // hb, step, 0)

    def upper(c):
        base, rb = (c - 1) * rc, 16
        lane = lax.broadcasted_iota(jnp.int32, (rb, 128), 1)
        sums = []
        for i in range(rc // rb):
            rows = pl.ds(base + i * rb, rb)
            acc = ru[0, rows, :].astype(f32)
            for s in range(1, n):
                acc = acc + ru[s, rows, :].astype(f32)
            acc = acc * rate
            totu[rows, :] = acc
            w = mu[rows, :]
            sums.append(
                jnp.where(
                    lane == 0,
                    jnp.sum(w * w, axis=1, keepdims=True),
                    jnp.sum(acc * acc, axis=1, keepdims=True),
                )
            )
        square = jnp.concatenate(sums * (128 // rc), axis=0)
        total = exchange(c, square.T[0:8, :])
        back = jnp.concatenate([total] * 16, axis=0).T
        scales = jnp.sqrt(back[:, 0:1]) * lax.rsqrt(back[:, 1:2] + 1e-06)
        for i in range(rc // rb):
            rows = pl.ds(base + i * rb, rb)
            state, stepped = update(
                totu[rows, :] * scales[i * rb : (i + 1) * rb, :], mu[rows, :], eu[rows, :]
            )
            tu[rows, :] = state
            su[rows, :] = stepped
            cu[pl.ds(up(me * R + base + i * rb, 16), rb), :] = stepped.astype(bf16)

    def az_copy(c, o):
        b = block_of(c, me)
        return remote(b, b, azs.at[c, o], azr.at[c, z], (lax.rem(z + o, Z) * Y + y, tp))

    def ay_copy(c, q, o):
        b = block_of(c, q * Y + y)
        return remote(b, b, ays.at[c, q, o], ayr.at[c, q, y], (z * Y + lax.rem(y + o, Y), tp))

    def gather_start(c):
        for o in range(1, Z):
            az_copy(c, o).start()
        for o in range(1, Y):
            ay_copy(c, z, o).start()

    def forward(c):
        for o in range(1, Z):
            q = lax.rem(z + o, Z)
            b = block_of(c, q * Y + y)
            remote(b, b, azs.at[c, 0], azr.at[c, q], (q * Y + y, tp)).wait_recv()
            for v in range(1, Y):
                ay_copy(c, q, v).start()

    def norm():
        for s in peers:
            remote(pn, rn.at[s], nms.at[0], nmr.at[s], (s, tp)).wait_recv()
        total = rn[0, 0:n, :]
        for s in range(1, n):
            total = total + rn[s, 0:n, :]
        master = jnp.concatenate([rn[s, n : n + 1, :] for s in range(n)], axis=0)
        memory = jnp.concatenate([rn[s, n + 1 : n + 2, :] for s in range(n)], axis=0)
        state, stepped = update(total * rate, master, memory)
        cn[...] = stepped.astype(bf16)
        line = lax.broadcasted_iota(jnp.int32, stepped.shape, 0)
        sn[...] = jnp.sum(jnp.where(line == me, stepped, 0.0), axis=0, keepdims=True)
        tn[...] = jnp.sum(jnp.where(line == me, state, 0.0), axis=0, keepdims=True)

    barrier = pltpu.get_barrier_semaphore()
    for d in peers:
        pl.semaphore_signal(barrier, inc=1, device_id=(d, tp), device_id_type=MESH)
    for t in tpeers:
        pl.semaphore_signal(barrier, inc=1, device_id=(me, t), device_id_type=MESH)
    for c in range(K + 1):
        local_copy(c).start()
    rn[me] = pn[...]
    pl.semaphore_wait(barrier, n + T - 2)

    rs_start(0)
    for o, d in enumerate(peers):
        remote(pn, rn.at[me], nms.at[o], nmr.at[me], (d, tp)).start()
    rs_start(1)
    norm()
    rs_wait(0)
    down()
    gather_start(0)
    for c in range(1, K + 1):
        if c < K:
            rs_start(c + 1)
        rs_wait(c)
        upper(c)
        gather_start(c)
        forward(c - 1)
    forward(K)

    for o, d in enumerate(peers):
        remote(pn, rn.at[me], nms.at[o], nmr.at[me], (d, tp)).wait_send()
    for c in range(K + 1):
        for o, d in enumerate(peers):
            rs_copy(c, o, d).wait_send()
        for o, t in enumerate(tpeers):
            nx_copy(c, o, t).wait_send()
        for o in range(1, Z):
            az_copy(c, o).wait_send()
        for q in range(Z):
            for o in range(1, Y):
                ay_copy(c, q, o).wait_send()
                v = lax.rem(y + o, Y)
                b = block_of(c, q * Y + v)
                remote(b, b, ays.at[c, q, 0], ayr.at[c, q, v], (z * Y + v, tp)).wait_recv()


def fused(pu, pd, pn, mu, md, mn, eu, ed, en):
    n, T = lax.axis_size("dp"), lax.axis_size("tp")
    Y = 2 if n % 2 == 0 else 1
    Z = n // Y
    (R, C), (H, W) = mu.shape, md.shape
    K = 2 if R % 32 == 0 else 1
    V = mn.shape[0]
    rows = -(-(n + 2) // 8) * 8
    packed = jnp.concatenate(
        [
            pn[0].astype(f32).reshape(n, V),
            mn[None],
            en[None],
            jnp.zeros((rows - n - 2, V), f32),
        ]
    )
    hbm = pl.BlockSpec(memory_space=pl.ANY)
    vmem = pl.BlockSpec(memory_space=pltpu.VMEM)
    shape = jax.ShapeDtypeStruct
    dma = pltpu.SemaphoreType.DMA
    outs = pl.pallas_call(
        functools.partial(kernel, n, T, Y, K),
        out_shape=(
            shape((H, n * W), bf16),
            shape((n * R, C), bf16),
            shape((n, V), bf16),
            shape((H, W), f32),
            shape((R, C), f32),
            shape((1, V), f32),
            shape((H, W), f32),
            shape((R, C), f32),
            shape((1, V), f32),
        ),
        in_specs=[hbm, hbm] + [vmem] * 5,
        out_specs=[vmem] * 9,
        scratch_shapes=[
            pltpu.VMEM((n, H, W), bf16),
            pltpu.VMEM((n, R, C), bf16),
            pltpu.VMEM((n, rows, V), f32),
            pltpu.VMEM((H, W), f32),
            pltpu.VMEM((R, C), f32),
            pltpu.VMEM((K + 1, 8, 128), f32),
            pltpu.VMEM((K + 1, T, 8, 128), f32),
            dma((K + 1,)),
            dma((n,)),
            dma((n,)),
            dma((K + 1, n)),
            dma((K + 1, n)),
            dma((K + 1, T)),
            dma((K + 1, T)),
            dma((K + 1, Z)),
            dma((K + 1, Z)),
            dma((K + 1, Z, Y)),
            dma((K + 1, Z, Y)),
        ],
        compiler_params=pltpu.CompilerParams(
            collective_id=0, has_side_effects=True, vmem_limit_bytes=56 * 1024 * 1024
        ),
    )(pd, pu, packed, md, ed, mu, eu)
    cd, cu, cn, sd, su, sn, td, tu, tn = outs
    return cu, cd, cn.reshape(-1), su, sd, sn.reshape(-1), tu, td, tn.reshape(-1)


def local(
    partial_up,
    partial_down,
    partial_norm,
    master_up,
    master_down,
    master_norm,
    memory_up,
    memory_down,
    memory_norm,
):
    mean_up, mean_down, mean_norm = (
        lax.psum_scatter(partial_up[0].astype(jnp.float32), "dp", scatter_dimension=0, tiled=True),
        lax.psum_scatter(
            partial_down[0].astype(jnp.float32), "dp", scatter_dimension=1, tiled=True
        ),
        lax.psum_scatter(
            partial_norm[0].astype(jnp.float32), "dp", scatter_dimension=0, tiled=True
        ),
    )
    mean_rate = lax.axis_size("dp") ** (-0.5)
    mean_up = mean_up * mean_rate
    mean_down = mean_down * mean_rate
    mean_norm = mean_norm * mean_rate
    own_up, own_down, slope_up_norm, slope_down_norm = lax.psum(
        (
            jnp.sum(master_up * master_up, axis=1, keepdims=True),
            jnp.sum(master_down * master_down, axis=0, keepdims=True),
            jnp.sum(mean_up * mean_up, axis=1, keepdims=True),
            jnp.sum(mean_down * mean_down, axis=0, keepdims=True),
        ),
        "tp",
    )
    mean_up = mean_up * (jnp.sqrt(own_up) * lax.rsqrt(slope_up_norm + 1e-06))
    mean_down = mean_down * (jnp.sqrt(own_down) * lax.rsqrt(slope_down_norm + 1e-06))
    state_new_up = hold_rate * memory_up + (1.0 - hold_rate) * mean_up * mean_up
    stepped_up = master_up - learn_rate * mean_up * lax.rsqrt(state_new_up + 1e-06)
    state_new_down = hold_rate * memory_down + (1.0 - hold_rate) * mean_down * mean_down
    stepped_down = master_down - learn_rate * mean_down * lax.rsqrt(state_new_down + 1e-06)
    state_new_norm = hold_rate * memory_norm + (1.0 - hold_rate) * mean_norm * mean_norm
    stepped_norm = master_norm - learn_rate * mean_norm * lax.rsqrt(state_new_norm + 1e-06)
    compute_up, compute_down, compute_norm = (
        lax.all_gather(stepped_up.astype(jnp.bfloat16), "dp", axis=0, tiled=True),
        lax.all_gather(stepped_down.astype(jnp.bfloat16), "dp", axis=1, tiled=True),
        lax.all_gather(stepped_norm.astype(jnp.bfloat16), "dp", axis=0, tiled=True),
    )
    return (
        compute_up,
        compute_down,
        compute_norm,
        stepped_up,
        stepped_down,
        stepped_norm,
        state_new_up,
        state_new_down,
        state_new_norm,
    )


def either(*args):
    (R, C), (H, W) = args[3].shape, args[4].shape
    V = args[5].shape[0]
    aligned = R == 128 and W == 128 and V == 128 and C % 128 == 0 and H % 128 == 0
    return fused(*args) if aligned else local(*args)


def solution(mesh):
    return jax.shard_map(
        either,
        mesh=mesh,
        in_specs=(
            P("dp", None, "tp"),
            P("dp", "tp", None),
            P("dp", None),
            P("dp", "tp"),
            P("tp", "dp"),
            P("dp"),
            P("dp", "tp"),
            P("tp", "dp"),
            P("dp"),
        ),
        out_specs=(
            P(None, "tp"),
            P("tp", None),
            P(),
            P("dp", "tp"),
            P("tp", "dp"),
            P("dp"),
            P("dp", "tp"),
            P("tp", "dp"),
            P("dp"),
        ),
        check_vma=False,
    )
```

```python
import functools

import jax
import jax.numpy as jnp
from jax import lax
from jax.experimental import pallas as pl
from jax.experimental.pallas import tpu as pltpu
from jax.sharding import PartitionSpec as P

learn_rate = 0.025
hold_rate = 0.8
f32 = jnp.float32
bf16 = jnp.bfloat16
MESH = pl.DeviceIdType.MESH


def kernel(
    n, T, Y, K,
    pd, pu, pn, md, ed, mu, eu,
    cd, cu, cn, sd, su, sn, td, tu, tn,
    od, yd, sumd, leftd, rightd, ou, yu, sumu, leftu, rightu,
    rn, totd, totu, nsend, nrecv,
    loc, nms, nmr, yss, ysr, zss, zlr, zrr, nxs, nxr, als, ars, azr, ays, ayr,
):
    Z = n // Y
    me = lax.axis_index("dp")
    tp = lax.axis_index("tp")
    z, y = me // Y, me % Y
    H, W = md.shape
    R = mu.shape[0]
    rc = R // K
    rate = n ** -0.5
    hb, rb = 128, 16
    order = list(range(K + 1))

    def remote(src, dst, s, r, dev):
        return pltpu.make_async_remote_copy(
            src_ref=src, dst_ref=dst, send_sem=s, recv_sem=r, device_id=dev, device_id_type=MESH
        )

    def up(a, m):
        return pl.multiple_of(a, m)

    peers = [lax.rem(me + o, n) for o in range(1, n)]
    tpeers = [lax.rem(tp + o, T) for o in range(1, T)]
    right, left = (lax.rem(z + 1, Z) * Y + y, tp), (lax.rem(z + Z - 1, Z) * Y + y, tp)
    other = (z * Y + lax.rem(y + 1, Y), tp)

    def src_of(c, d):
        if c == 0:
            return pd.at[0, :, pl.ds(up(d * W, 128), W)]
        return pu.at[0, pl.ds(up(d * R + (c - 1) * rc, 16), rc), :]

    def slot(c, down_ref, up_ref, q):
        if c == 0:
            return down_ref.at[q]
        return up_ref.at[q, pl.ds((c - 1) * rc, rc), :]

    def block_of(c, d):
        if c == 0:
            return cd.at[:, pl.ds(up(d * W, 128), W)]
        return cu.at[pl.ds(up(d * R + (c - 1) * rc, 16), rc), :]

    def rows_of(c, i):
        if c == 0:
            return pl.ds(up(i * hb, hb), hb)
        return pl.ds(up((c - 1) * rc + i * rb, rb), rb)

    def count(c):
        return H // hb if c == 0 else rc // rb

    def local_copy(c, q):
        return pltpu.make_async_copy(src_of(c, q * Y + y), slot(c, od, ou, q), loc.at[c, q])

    def y_copy(c, q):
        d = q * Y + lax.rem(y + 1, Y)
        return remote(src_of(c, d), slot(c, yd, yu, q), yss.at[c, q], ysr.at[c, q], other)

    def y_wait(c, q):
        local_copy(c, q).wait()
        if Y > 1:
            y_copy(c, q).wait_recv()

    def y_start(c, qs):
        for q in qs:
            local_copy(c, q).start()
            if Y > 1:
                y_copy(c, q).start()

    def pair(c, q, rows):
        o, v = (od, yd) if c == 0 else (ou, yu)
        total = o[q, rows, :].astype(f32)
        if Y > 1:
            total = total + v[q, rows, :].astype(f32)
        return total

    def to_right(c, q):
        return remote(slot(c, sumd, sumu, q), slot(c, leftd, leftu, q), zss.at[c, q], zlr.at[c, q], right)

    def to_left(c, q):
        return remote(slot(c, sumd, sumu, q), slot(c, rightd, rightu, q), zss.at[c, q], zrr.at[c, q], left)

    def relay(c, q, rightward, first):
        out = sumd if c == 0 else sumu
        y_wait(c, q)
        if rightward:
            held = leftd if c == 0 else leftu
            if not first:
                to_right(c, q).wait_recv()
        else:
            held = rightd if c == 0 else rightu
            if not first:
                to_left(c, q).wait_recv()

        def add(i, carry):
            rows = rows_of(c, i)
            total = pair(c, q, rows)
            if not first:
                total = total + held[q, rows, :]
            out[q, rows, :] = total
            return carry

        lax.fori_loop(0, count(c), add, 0)
        (to_right if rightward else to_left)(c, q).start()

    def ends(c):
        if Z == 1:
            return

        @pl.when(z == 0)
        def _():
            for q in range(Z - 1, 0, -1):
                relay(c, q, True, True)

        @pl.when(z == Z - 1)
        def _():
            for q in range(Z - 1):
                relay(c, q, False, True)

    def middle(c):
        for k in range(Z - 1):
            q = Z - 1 - k

            @pl.when((z > 0) & (z < q))
            def _():
                relay(c, q, True, False)

            @pl.when((z < Z - 1) & (z > k))
            def _():
                relay(c, k, False, False)

    def final_wait(c):
        y_wait(c, z)

        @pl.when(z > 0)
        def _():
            to_right(c, z).wait_recv()

        @pl.when(z < Z - 1)
        def _():
            to_left(c, z).wait_recv()

    def whole(c, rows):
        l, r = (leftd, rightd) if c == 0 else (leftu, rightu)
        total = pair(c, z, rows)
        total = total + jnp.where(z > 0, l[z, rows, :], 0.0)
        total = total + jnp.where(z < Z - 1, r[z, rows, :], 0.0)
        return total * rate

    def nx_copy(c, o, t):
        return remote(nsend.at[c], nrecv.at[c, tp], nxs.at[c, o], nxr.at[c, tp], (me, t))

    def exchange(c, value):
        nsend[c] = value
        nrecv[c, tp] = value
        for o, t in enumerate(tpeers):
            nx_copy(c, o, t).start()
        for t in tpeers:
            remote(nsend.at[c], nrecv.at[c, t], nxs.at[c, 0], nxr.at[c, t], (me, t)).wait_recv()
        total = nrecv[c, 0]
        for t in range(1, T):
            total = total + nrecv[c, t]
        return total

    def update(m, master, memory):
        state = hold_rate * memory + (1.0 - hold_rate) * m * m
        return state, master - learn_rate * m * lax.rsqrt(state + 1e-06)

    def down():
        c = 0

        def add(i, carry):
            rows = rows_of(c, i)
            acc = whole(c, rows)
            totd[rows, :] = acc
            w = md[rows, :]
            return (
                carry[0] + jnp.sum((w * w).reshape(hb // 8, 8, W), axis=0),
                carry[1] + jnp.sum((acc * acc).reshape(hb // 8, 8, W), axis=0),
            )

        zero = jnp.zeros((8, W), f32)
        own, slope = lax.fori_loop(0, H // hb, add, (zero, zero))
        own = jnp.sum(own, axis=0, keepdims=True)
        slope = jnp.sum(slope, axis=0, keepdims=True)
        line = lax.broadcasted_iota(jnp.int32, (8, W), 0)
        total = exchange(c, jnp.where(line == 0, own, slope))
        scale = jnp.sqrt(total[0:1, :]) * lax.rsqrt(total[1:2, :] + 1e-06)

        def step(i, carry):
            rows = rows_of(c, i)
            state, stepped = update(totd[rows, :] * scale, md[rows, :], ed[rows, :])
            td[rows, :] = state
            sd[rows, :] = stepped
            cd[rows, pl.ds(up(me * W, 128), W)] = stepped.astype(bf16)
            return carry

        lax.fori_loop(0, H // hb, step, 0)

    def upper(c):
        lane = lax.broadcasted_iota(jnp.int32, (rb, 128), 1)
        sums = []
        for i in range(rc // rb):
            rows = rows_of(c, i)
            acc = whole(c, rows)
            totu[rows, :] = acc
            w = mu[rows, :]
            sums.append(
                jnp.where(
                    lane == 0,
                    jnp.sum(w * w, axis=1, keepdims=True),
                    jnp.sum(acc * acc, axis=1, keepdims=True),
                )
            )
        square = jnp.concatenate(sums * (128 // rc), axis=0)
        total = exchange(c, square.T[0:8, :])
        back = jnp.concatenate([total] * 16, axis=0).T
        scales = jnp.sqrt(back[:, 0:1]) * lax.rsqrt(back[:, 1:2] + 1e-06)
        for i in range(rc // rb):
            rows = rows_of(c, i)
            state, stepped = update(
                totu[rows, :] * scales[i * rb : (i + 1) * rb, :], mu[rows, :], eu[rows, :]
            )
            tu[rows, :] = state
            su[rows, :] = stepped
            cu[pl.ds(up(me * R + (c - 1) * rc + i * rb, 16), rb), :] = stepped.astype(bf16)

    def final(c):
        final_wait(c)
        if c == 0:
            down()
        else:
            upper(c)

    def move(c, q, s, dev):
        b = block_of(c, q * Y + y)
        return remote(b, b, s.at[c, q], azr.at[c, q], dev)

    def y_move(c, q, v):
        b = block_of(c, q * Y + v)
        return remote(b, b, ays.at[c, q], ayr.at[c, q], other)

    def gather_start(c):
        @pl.when(z < Z - 1)
        def _():
            move(c, z, ars, right).start()

        @pl.when(z > 0)
        def _():
            move(c, z, als, left).start()

        if Y > 1:
            y_move(c, z, y).start()

    def forward(c):
        for k in range(1, Z):
            @pl.when(z >= k)
            def _():
                q = z - k
                move(c, q, ars, right).wait_recv()

                @pl.when(z < Z - 1)
                def _():
                    move(c, q, ars, right).start()

                if Y > 1:
                    y_move(c, q, y).start()

            @pl.when(z + k < Z)
            def _():
                q = z + k
                move(c, q, als, left).wait_recv()

                @pl.when(z > 0)
                def _():
                    move(c, q, als, left).start()

                if Y > 1:
                    y_move(c, q, y).start()

    def norm():
        for s in peers:
            remote(pn, rn.at[s], nms.at[0], nmr.at[s], (s, tp)).wait_recv()
        total = rn[0, 0:n, :]
        for s in range(1, n):
            total = total + rn[s, 0:n, :]
        master = jnp.concatenate([rn[s, n : n + 1, :] for s in range(n)], axis=0)
        memory = jnp.concatenate([rn[s, n + 1 : n + 2, :] for s in range(n)], axis=0)
        state, stepped = update(total * rate, master, memory)
        cn[...] = stepped.astype(bf16)
        line = lax.broadcasted_iota(jnp.int32, stepped.shape, 0)
        sn[...] = jnp.sum(jnp.where(line == me, stepped, 0.0), axis=0, keepdims=True)
        tn[...] = jnp.sum(jnp.where(line == me, state, 0.0), axis=0, keepdims=True)

    barrier = pltpu.get_barrier_semaphore()
    for d in peers:
        pl.semaphore_signal(barrier, inc=1, device_id=(d, tp), device_id_type=MESH)
    for t in tpeers:
        pl.semaphore_signal(barrier, inc=1, device_id=(me, t), device_id_type=MESH)
    rn[me] = pn[...]
    pl.semaphore_wait(barrier, n + T - 2)

    far = []
    for k in range((Z + 1) // 2):
        far += [Z - 1 - k] + ([k] if k != Z - 1 - k else [])

    @pl.when(2 * z < Z)
    def _():
        for c in order:
            y_start(c, far)

    @pl.when(2 * z >= Z)
    def _():
        for c in order:
            y_start(c, [Z - 1 - q for q in far])

    for o, d in enumerate(peers):
        remote(pn, rn.at[me], nms.at[o], nmr.at[me], (d, tp)).start()

    ends(order[0])
    middle(order[0])
    for i, c in enumerate(order):
        last = i + 1 == len(order)
        if not last:
            ends(order[i + 1])
        if i >= 1:
            forward(order[i - 1])
        final(c)
        gather_start(c)
        if i == 0:
            norm()
        if not last:
            middle(order[i + 1])
    forward(order[-1])

    for o, d in enumerate(peers):
        remote(pn, rn.at[me], nms.at[o], nmr.at[me], (d, tp)).wait_send()
    for c in order:
        for o, t in enumerate(tpeers):
            nx_copy(c, o, t).wait_send()
        for q in range(Z):
            if Y > 1:
                y_copy(c, q).wait_send()
                y_move(c, q, y).wait_send()
                y_move(c, q, lax.rem(y + 1, Y)).wait_recv()

            @pl.when(z != q)
            def _():
                to_right(c, q).wait_send()

            @pl.when((z >= q) & (z < Z - 1))
            def _():
                move(c, q, ars, right).wait_send()

            @pl.when((z <= q) & (z > 0))
            def _():
                move(c, q, als, left).wait_send()


def fused(pu, pd, pn, mu, md, mn, eu, ed, en):
    n, T = lax.axis_size("dp"), lax.axis_size("tp")
    Y = 2 if n % 2 == 0 else 1
    Z = n // Y
    (R, C), (H, W) = mu.shape, md.shape
    K = 2 if R % 32 == 0 else 1
    V = mn.shape[0]
    rows = -(-(n + 2) // 8) * 8
    packed = jnp.concatenate(
        [
            pn[0].astype(f32).reshape(n, V),
            mn[None],
            en[None],
            jnp.zeros((rows - n - 2, V), f32),
        ]
    )
    hbm = pl.BlockSpec(memory_space=pl.ANY)
    vmem = pl.BlockSpec(memory_space=pltpu.VMEM)
    shape = jax.ShapeDtypeStruct
    dma = pltpu.SemaphoreType.DMA
    outs = pl.pallas_call(
        functools.partial(kernel, n, T, Y, K),
        out_shape=(
            shape((H, n * W), bf16),
            shape((n * R, C), bf16),
            shape((n, V), bf16),
            shape((H, W), f32),
            shape((R, C), f32),
            shape((1, V), f32),
            shape((H, W), f32),
            shape((R, C), f32),
            shape((1, V), f32),
        ),
        in_specs=[hbm, hbm] + [vmem] * 5,
        out_specs=[vmem] * 9,
        scratch_shapes=[
            pltpu.VMEM((Z, H, W), bf16),
            pltpu.VMEM((Z, H, W), bf16),
            pltpu.VMEM((Z, H, W), f32),
            pltpu.VMEM((Z, H, W), f32),
            pltpu.VMEM((Z, H, W), f32),
            pltpu.VMEM((Z, R, C), bf16),
            pltpu.VMEM((Z, R, C), bf16),
            pltpu.VMEM((Z, R, C), f32),
            pltpu.VMEM((Z, R, C), f32),
            pltpu.VMEM((Z, R, C), f32),
            pltpu.VMEM((n, rows, V), f32),
            pltpu.VMEM((H, W), f32),
            pltpu.VMEM((R, C), f32),
            pltpu.VMEM((K + 1, 8, 128), f32),
            pltpu.VMEM((K + 1, T, 8, 128), f32),
            dma((K + 1, Z)),
            dma((n,)),
            dma((n,)),
            dma((K + 1, Z)),
            dma((K + 1, Z)),
            dma((K + 1, Z)),
            dma((K + 1, Z)),
            dma((K + 1, Z)),
            dma((K + 1, T)),
            dma((K + 1, T)),
            dma((K + 1, Z)),
            dma((K + 1, Z)),
            dma((K + 1, Z)),
            dma((K + 1, Z)),
            dma((K + 1, Z)),
        ],
        compiler_params=pltpu.CompilerParams(
            collective_id=0, has_side_effects=True, vmem_limit_bytes=56 * 1024 * 1024
        ),
    )(pd, pu, packed, md, ed, mu, eu)
    cd, cu, cn, sd, su, sn, td, tu, tn = outs
    return cu, cd, cn.reshape(-1), su, sd, sn.reshape(-1), tu, td, tn.reshape(-1)


def local(
    partial_up,
    partial_down,
    partial_norm,
    master_up,
    master_down,
    master_norm,
    memory_up,
    memory_down,
    memory_norm,
):
    mean_up, mean_down, mean_norm = (
        lax.psum_scatter(partial_up[0].astype(jnp.float32), "dp", scatter_dimension=0, tiled=True),
        lax.psum_scatter(
            partial_down[0].astype(jnp.float32), "dp", scatter_dimension=1, tiled=True
        ),
        lax.psum_scatter(
            partial_norm[0].astype(jnp.float32), "dp", scatter_dimension=0, tiled=True
        ),
    )
    mean_rate = lax.axis_size("dp") ** (-0.5)
    mean_up = mean_up * mean_rate
    mean_down = mean_down * mean_rate
    mean_norm = mean_norm * mean_rate
    own_up, own_down, slope_up_norm, slope_down_norm = lax.psum(
        (
            jnp.sum(master_up * master_up, axis=1, keepdims=True),
            jnp.sum(master_down * master_down, axis=0, keepdims=True),
            jnp.sum(mean_up * mean_up, axis=1, keepdims=True),
            jnp.sum(mean_down * mean_down, axis=0, keepdims=True),
        ),
        "tp",
    )
    mean_up = mean_up * (jnp.sqrt(own_up) * lax.rsqrt(slope_up_norm + 1e-06))
    mean_down = mean_down * (jnp.sqrt(own_down) * lax.rsqrt(slope_down_norm + 1e-06))
    state_new_up = hold_rate * memory_up + (1.0 - hold_rate) * mean_up * mean_up
    stepped_up = master_up - learn_rate * mean_up * lax.rsqrt(state_new_up + 1e-06)
    state_new_down = hold_rate * memory_down + (1.0 - hold_rate) * mean_down * mean_down
    stepped_down = master_down - learn_rate * mean_down * lax.rsqrt(state_new_down + 1e-06)
    state_new_norm = hold_rate * memory_norm + (1.0 - hold_rate) * mean_norm * mean_norm
    stepped_norm = master_norm - learn_rate * mean_norm * lax.rsqrt(state_new_norm + 1e-06)
    compute_up, compute_down, compute_norm = (
        lax.all_gather(stepped_up.astype(jnp.bfloat16), "dp", axis=0, tiled=True),
        lax.all_gather(stepped_down.astype(jnp.bfloat16), "dp", axis=1, tiled=True),
        lax.all_gather(stepped_norm.astype(jnp.bfloat16), "dp", axis=0, tiled=True),
    )
    return (
        compute_up,
        compute_down,
        compute_norm,
        stepped_up,
        stepped_down,
        stepped_norm,
        state_new_up,
        state_new_down,
        state_new_norm,
    )


def either(*args):
    (R, C), (H, W) = args[3].shape, args[4].shape
    V = args[5].shape[0]
    aligned = R == 128 and W == 128 and V == 128 and C % 128 == 0 and H % 128 == 0
    return fused(*args) if aligned else local(*args)


def solution(mesh):
    return jax.shard_map(
        either,
        mesh=mesh,
        in_specs=(
            P("dp", None, "tp"),
            P("dp", "tp", None),
            P("dp", None),
            P("dp", "tp"),
            P("tp", "dp"),
            P("dp"),
            P("dp", "tp"),
            P("tp", "dp"),
            P("dp"),
        ),
        out_specs=(
            P(None, "tp"),
            P("tp", None),
            P(),
            P("dp", "tp"),
            P("tp", "dp"),
            P("dp"),
            P("dp", "tp"),
            P("tp", "dp"),
            P("dp"),
        ),
        check_vma=False,
    )
```

```python
import functools

import jax
import jax.numpy as jnp
from jax import lax
from jax.experimental import pallas as pl
from jax.experimental.pallas import tpu as pltpu
from jax.sharding import PartitionSpec as P

learn_rate = 0.025
hold_rate = 0.8
f32 = jnp.float32
bf16 = jnp.bfloat16
MESH = pl.DeviceIdType.MESH


def schedule(D, K):
    downs, ups = list(range(D)), list(range(D, D + K))
    plan = [('end', 1), ('end', 0), ('mid', 1), ('sum', (1,)), ('end', 2), ('mid', 0), ('fwd', 1), ('sum', (0,)), ('mid', 2), ('fwd', 0), ('sum', (2,)), ('fwd', 2)]
    return plan


def kernel(
    n, T, Y, D, K,
    pd, pu, pn, md, ed, mu, eu,
    cd, cu, cn, sd, su, sn, td, tu, tn,
    od, yd, sumd, leftd, rightd, ou, yu, sumu, leftu, rightu,
    rn, totd, totu, nsend, nrecv,
    loc, nms, nmr, yss, ysr, zss, zlr, zrr, nxs, nxr, als, ars, azr, ays, ayr,
):
    Z = n // Y
    me = lax.axis_index("dp")
    tp = lax.axis_index("tp")
    z, y = me // Y, me % Y
    H, W = md.shape
    R = mu.shape[0]
    rc = R // K
    rate = n ** -0.5
    hb, rb = 128, 16
    hc = H // D
    plan = schedule(D, K)
    order = [p for op, p in plan if op == "end"]

    def remote(src, dst, s, r, dev):
        return pltpu.make_async_remote_copy(
            src_ref=src, dst_ref=dst, send_sem=s, recv_sem=r, device_id=dev, device_id_type=MESH
        )

    def up(a, m):
        return pl.multiple_of(a, m)

    peers = [lax.rem(me + o, n) for o in range(1, n)]
    tpeers = [lax.rem(tp + o, T) for o in range(1, T)]
    right, left = (lax.rem(z + 1, Z) * Y + y, tp), (lax.rem(z + Z - 1, Z) * Y + y, tp)
    other = (z * Y + lax.rem(y + 1, Y), tp)

    def src_of(c, d):
        if c < D:
            return pd.at[0, pl.ds(c * hc, hc), pl.ds(up(d * W, 128), W)]
        return pu.at[0, pl.ds(up(d * R + (c - D) * rc, 16), rc), :]

    def slot(c, down_ref, up_ref, q):
        if c < D:
            return down_ref.at[q, pl.ds(c * hc, hc), :]
        return up_ref.at[q, pl.ds((c - D) * rc, rc), :]

    def block_of(c, d):
        if c < D:
            return cd.at[pl.ds(c * hc, hc), pl.ds(up(d * W, 128), W)]
        return cu.at[pl.ds(up(d * R + (c - D) * rc, 16), rc), :]

    def rows_of(c, i):
        if c < D:
            return pl.ds(up(c * hc + i * hb, hb), hb)
        return pl.ds(up((c - D) * rc + i * rb, rb), rb)

    def count(c):
        return hc // hb if c < D else rc // rb

    def local_copy(c, q):
        return pltpu.make_async_copy(src_of(c, q * Y + y), slot(c, od, ou, q), loc.at[c, q])

    def y_copy(c, q):
        d = q * Y + lax.rem(y + 1, Y)
        return remote(src_of(c, d), slot(c, yd, yu, q), yss.at[c, q], ysr.at[c, q], other)

    def y_wait(c, q):
        local_copy(c, q).wait()
        if Y > 1:
            y_copy(c, q).wait_recv()

    def y_start(c, qs):
        for q in qs:
            local_copy(c, q).start()
            if Y > 1:
                y_copy(c, q).start()

    def pair(c, q, rows):
        o, v = (od, yd) if c < D else (ou, yu)
        total = o[q, rows, :].astype(f32)
        if Y > 1:
            total = total + v[q, rows, :].astype(f32)
        return total

    def to_right(c, q):
        return remote(slot(c, sumd, sumu, q), slot(c, leftd, leftu, q), zss.at[c, q], zlr.at[c, q], right)

    def to_left(c, q):
        return remote(slot(c, sumd, sumu, q), slot(c, rightd, rightu, q), zss.at[c, q], zrr.at[c, q], left)

    def relay(c, q, rightward, first):
        out = sumd if c < D else sumu
        y_wait(c, q)
        if rightward:
            held = leftd if c < D else leftu
            if not first:
                to_right(c, q).wait_recv()
        else:
            held = rightd if c < D else rightu
            if not first:
                to_left(c, q).wait_recv()

        def add(i, carry):
            rows = rows_of(c, i)
            total = pair(c, q, rows)
            if not first:
                total = total + held[q, rows, :]
            out[q, rows, :] = total
            return carry

        lax.fori_loop(0, count(c), add, 0)
        (to_right if rightward else to_left)(c, q).start()

    def ends(c):
        if Z == 1:
            return

        @pl.when(z == 0)
        def _():
            for q in range(Z - 1, 0, -1):
                relay(c, q, True, True)

        @pl.when(z == Z - 1)
        def _():
            for q in range(Z - 1):
                relay(c, q, False, True)

    def middle(c):
        for k in range(Z - 1):
            q = Z - 1 - k

            @pl.when((z > 0) & (z < q))
            def _():
                relay(c, q, True, False)

            @pl.when((z < Z - 1) & (z > k))
            def _():
                relay(c, k, False, False)

    def final_wait(c):
        y_wait(c, z)

        @pl.when(z > 0)
        def _():
            to_right(c, z).wait_recv()

        @pl.when(z < Z - 1)
        def _():
            to_left(c, z).wait_recv()

    def whole(c, rows):
        l, r = (leftd, rightd) if c < D else (leftu, rightu)
        total = pair(c, z, rows)
        total = total + jnp.where(z > 0, l[z, rows, :], 0.0)
        total = total + jnp.where(z < Z - 1, r[z, rows, :], 0.0)
        return total * rate

    def nx_copy(c, o, t):
        return remote(nsend.at[c], nrecv.at[c, tp], nxs.at[c, o], nxr.at[c, tp], (me, t))

    def exchange(c, value):
        nsend[c] = value
        nrecv[c, tp] = value
        for o, t in enumerate(tpeers):
            nx_copy(c, o, t).start()
        for t in tpeers:
            remote(nsend.at[c], nrecv.at[c, t], nxs.at[c, 0], nxr.at[c, t], (me, t)).wait_recv()
        total = nrecv[c, 0]
        for t in range(1, T):
            total = total + nrecv[c, t]
        return total

    def update(m, master, memory):
        state = hold_rate * memory + (1.0 - hold_rate) * m * m
        return state, master - learn_rate * m * lax.rsqrt(state + 1e-06)

    def down():
        c = 0

        def add(i, carry):
            rows = pl.ds(up(i * hb, hb), hb)
            acc = whole(c, rows)
            totd[rows, :] = acc
            w = md[rows, :]
            return (
                carry[0] + jnp.sum((w * w).reshape(hb // 8, 8, W), axis=0),
                carry[1] + jnp.sum((acc * acc).reshape(hb // 8, 8, W), axis=0),
            )

        zero = jnp.zeros((8, W), f32)
        own, slope = lax.fori_loop(0, H // hb, add, (zero, zero))
        own = jnp.sum(own, axis=0, keepdims=True)
        slope = jnp.sum(slope, axis=0, keepdims=True)
        line = lax.broadcasted_iota(jnp.int32, (8, W), 0)
        total = exchange(c, jnp.where(line == 0, own, slope))
        scale = jnp.sqrt(total[0:1, :]) * lax.rsqrt(total[1:2, :] + 1e-06)

        def step(i, carry):
            rows = pl.ds(up(i * hb, hb), hb)
            state, stepped = update(totd[rows, :] * scale, md[rows, :], ed[rows, :])
            td[rows, :] = state
            sd[rows, :] = stepped
            cd[rows, pl.ds(up(me * W, 128), W)] = stepped.astype(bf16)
            return carry

        lax.fori_loop(0, H // hb, step, 0)

    def upper(c):
        lane = lax.broadcasted_iota(jnp.int32, (rb, 128), 1)
        sums = []
        for i in range(rc // rb):
            rows = rows_of(c, i)
            acc = whole(c, rows)
            totu[rows, :] = acc
            w = mu[rows, :]
            sums.append(
                jnp.where(
                    lane == 0,
                    jnp.sum(w * w, axis=1, keepdims=True),
                    jnp.sum(acc * acc, axis=1, keepdims=True),
                )
            )
        square = jnp.concatenate(sums * (128 // rc), axis=0)
        total = exchange(c - D + 1, square.T[0:8, :])
        back = jnp.concatenate([total] * 16, axis=0).T
        scales = jnp.sqrt(back[:, 0:1]) * lax.rsqrt(back[:, 1:2] + 1e-06)
        for i in range(rc // rb):
            rows = rows_of(c, i)
            state, stepped = update(
                totu[rows, :] * scales[i * rb : (i + 1) * rb, :], mu[rows, :], eu[rows, :]
            )
            tu[rows, :] = state
            su[rows, :] = stepped
            cu[pl.ds(up(me * R + (c - D) * rc + i * rb, 16), rb), :] = stepped.astype(bf16)

    def final(unit):
        for c in unit:
            final_wait(c)
        if unit[0] < D:
            down()
        else:
            upper(unit[0])
        for c in unit:
            gather_start(c)

    def move(c, q, s, dev):
        b = block_of(c, q * Y + y)
        return remote(b, b, s.at[c, q], azr.at[c, q], dev)

    def y_move(c, q, v):
        b = block_of(c, q * Y + v)
        return remote(b, b, ays.at[c, q], ayr.at[c, q], other)

    def gather_start(c):
        @pl.when(z < Z - 1)
        def _():
            move(c, z, ars, right).start()

        @pl.when(z > 0)
        def _():
            move(c, z, als, left).start()

        if Y > 1:
            y_move(c, z, y).start()

    def forward(c):
        for k in range(1, Z):
            @pl.when(z >= k)
            def _():
                q = z - k
                move(c, q, ars, right).wait_recv()

                @pl.when(z < Z - 1)
                def _():
                    move(c, q, ars, right).start()

                if Y > 1:
                    y_move(c, q, y).start()

            @pl.when(z + k < Z)
            def _():
                q = z + k
                move(c, q, als, left).wait_recv()

                @pl.when(z > 0)
                def _():
                    move(c, q, als, left).start()

                if Y > 1:
                    y_move(c, q, y).start()

    def norm():
        for s in peers:
            remote(pn, rn.at[s], nms.at[0], nmr.at[s], (s, tp)).wait_recv()
        total = rn[0, 0:n, :]
        for s in range(1, n):
            total = total + rn[s, 0:n, :]
        master = jnp.concatenate([rn[s, n : n + 1, :] for s in range(n)], axis=0)
        memory = jnp.concatenate([rn[s, n + 1 : n + 2, :] for s in range(n)], axis=0)
        state, stepped = update(total * rate, master, memory)
        cn[...] = stepped.astype(bf16)
        line = lax.broadcasted_iota(jnp.int32, stepped.shape, 0)
        sn[...] = jnp.sum(jnp.where(line == me, stepped, 0.0), axis=0, keepdims=True)
        tn[...] = jnp.sum(jnp.where(line == me, state, 0.0), axis=0, keepdims=True)

    barrier = pltpu.get_barrier_semaphore()
    for d in peers:
        pl.semaphore_signal(barrier, inc=1, device_id=(d, tp), device_id_type=MESH)
    for t in tpeers:
        pl.semaphore_signal(barrier, inc=1, device_id=(me, t), device_id_type=MESH)
    rn[me] = pn[...]
    pl.semaphore_wait(barrier, n + T - 2)

    for o, d in enumerate(peers):
        remote(pn, rn.at[me], nms.at[o], nmr.at[me], (d, tp)).start()

    far = []
    for k in range((Z + 1) // 2):
        far += [Z - 1 - k] + ([k] if k != Z - 1 - k else [])

    @pl.when(2 * z < Z)
    def _():
        for c in order:
            y_start(c, far)

    @pl.when(2 * z >= Z)
    def _():
        for c in order:
            y_start(c, [Z - 1 - q for q in far])

    acts = {"end": ends, "mid": middle, "sum": final, "fwd": forward}
    for i, (op, p) in enumerate(plan):
        acts[op](p)
        if i + 2 == len(plan):
            norm()

    for o, d in enumerate(peers):
        remote(pn, rn.at[me], nms.at[o], nmr.at[me], (d, tp)).wait_send()
    for c in range(K + 1):
        for o, t in enumerate(tpeers):
            nx_copy(c, o, t).wait_send()
    for c in order:
        for q in range(Z):
            if Y > 1:
                y_copy(c, q).wait_send()
                y_move(c, q, y).wait_send()
                y_move(c, q, lax.rem(y + 1, Y)).wait_recv()

            @pl.when(z != q)
            def _():
                to_right(c, q).wait_send()

            @pl.when((z >= q) & (z < Z - 1))
            def _():
                move(c, q, ars, right).wait_send()

            @pl.when((z <= q) & (z > 0))
            def _():
                move(c, q, als, left).wait_send()


def finish(*refs):
    sems = refs[18]
    copies = [pltpu.make_async_copy(refs[i], refs[9 + i], sems.at[i]) for i in range(9)]
    for c in copies:
        c.start()
    for c in copies:
        c.wait()


def fused(pu, pd, pn, mu, md, mn, eu, ed, en):
    n, T = lax.axis_size("dp"), lax.axis_size("tp")
    Y = 2 if n % 2 == 0 else 1
    Z = n // Y
    (R, C), (H, W) = mu.shape, md.shape
    K = 2 if R % 32 == 0 else 1
    D = 1 if H % (1 * 128) == 0 else 1
    V = mn.shape[0]
    rows = -(-(n + 2) // 8) * 8
    packed = jnp.concatenate(
        [
            pn[0].astype(f32).reshape(n, V),
            mn[None],
            en[None],
            jnp.zeros((rows - n - 2, V), f32),
        ]
    )
    hbm = pl.BlockSpec(memory_space=pl.ANY)
    vmem = pl.BlockSpec(memory_space=pltpu.VMEM)
    shape = jax.ShapeDtypeStruct
    dma = pltpu.SemaphoreType.DMA
    outs = pl.pallas_call(
        functools.partial(kernel, n, T, Y, D, K),
        out_shape=(
            shape((H, n * W), bf16),
            shape((n * R, C), bf16),
            shape((n, V), bf16),
            shape((H, W), f32),
            shape((R, C), f32),
            shape((1, V), f32),
            shape((H, W), f32),
            shape((R, C), f32),
            shape((1, V), f32),
        ),
        in_specs=[hbm, hbm] + [vmem] * 5,
        out_specs=[vmem] * 9,
        scratch_shapes=[
            pltpu.VMEM((Z, H, W), bf16),
            pltpu.VMEM((Z, H, W), bf16),
            pltpu.VMEM((Z, H, W), f32),
            pltpu.VMEM((Z, H, W), f32),
            pltpu.VMEM((Z, H, W), f32),
            pltpu.VMEM((Z, R, C), bf16),
            pltpu.VMEM((Z, R, C), bf16),
            pltpu.VMEM((Z, R, C), f32),
            pltpu.VMEM((Z, R, C), f32),
            pltpu.VMEM((Z, R, C), f32),
            pltpu.VMEM((n, rows, V), f32),
            pltpu.VMEM((H, W), f32),
            pltpu.VMEM((R, C), f32),
            pltpu.VMEM((K + 1, 8, 128), f32),
            pltpu.VMEM((K + 1, T, 8, 128), f32),
            dma((D + K, Z)),
            dma((n,)),
            dma((n,)),
            dma((D + K, Z)),
            dma((D + K, Z)),
            dma((D + K, Z)),
            dma((D + K, Z)),
            dma((D + K, Z)),
            dma((K + 1, T)),
            dma((K + 1, T)),
            dma((D + K, Z)),
            dma((D + K, Z)),
            dma((D + K, Z)),
            dma((D + K, Z)),
            dma((D + K, Z)),
        ],
        compiler_params=pltpu.CompilerParams(
            collective_id=0, has_side_effects=True, vmem_limit_bytes=56 * 1024 * 1024
        ),
    )(pd, pu, packed, md, ed, mu, eu)
    outs = pl.pallas_call(
        finish,
        out_shape=[shape(o.shape, o.dtype) for o in outs],
        in_specs=[vmem] * 9,
        out_specs=[hbm] * 9,
        scratch_shapes=[dma((9,))],
    )(*outs)
    cd, cu, cn, sd, su, sn, td, tu, tn = outs
    return cu, cd, cn.reshape(-1), su, sd, sn.reshape(-1), tu, td, tn.reshape(-1)


def local(
    partial_up,
    partial_down,
    partial_norm,
    master_up,
    master_down,
    master_norm,
    memory_up,
    memory_down,
    memory_norm,
):
    mean_up, mean_down, mean_norm = (
        lax.psum_scatter(partial_up[0].astype(jnp.float32), "dp", scatter_dimension=0, tiled=True),
        lax.psum_scatter(
            partial_down[0].astype(jnp.float32), "dp", scatter_dimension=1, tiled=True
        ),
        lax.psum_scatter(
            partial_norm[0].astype(jnp.float32), "dp", scatter_dimension=0, tiled=True
        ),
    )
    mean_rate = lax.axis_size("dp") ** (-0.5)
    mean_up = mean_up * mean_rate
    mean_down = mean_down * mean_rate
    mean_norm = mean_norm * mean_rate
    own_up, own_down, slope_up_norm, slope_down_norm = lax.psum(
        (
            jnp.sum(master_up * master_up, axis=1, keepdims=True),
            jnp.sum(master_down * master_down, axis=0, keepdims=True),
            jnp.sum(mean_up * mean_up, axis=1, keepdims=True),
            jnp.sum(mean_down * mean_down, axis=0, keepdims=True),
        ),
        "tp",
    )
    mean_up = mean_up * (jnp.sqrt(own_up) * lax.rsqrt(slope_up_norm + 1e-06))
    mean_down = mean_down * (jnp.sqrt(own_down) * lax.rsqrt(slope_down_norm + 1e-06))
    state_new_up = hold_rate * memory_up + (1.0 - hold_rate) * mean_up * mean_up
    stepped_up = master_up - learn_rate * mean_up * lax.rsqrt(state_new_up + 1e-06)
    state_new_down = hold_rate * memory_down + (1.0 - hold_rate) * mean_down * mean_down
    stepped_down = master_down - learn_rate * mean_down * lax.rsqrt(state_new_down + 1e-06)
    state_new_norm = hold_rate * memory_norm + (1.0 - hold_rate) * mean_norm * mean_norm
    stepped_norm = master_norm - learn_rate * mean_norm * lax.rsqrt(state_new_norm + 1e-06)
    compute_up, compute_down, compute_norm = (
        lax.all_gather(stepped_up.astype(jnp.bfloat16), "dp", axis=0, tiled=True),
        lax.all_gather(stepped_down.astype(jnp.bfloat16), "dp", axis=1, tiled=True),
        lax.all_gather(stepped_norm.astype(jnp.bfloat16), "dp", axis=0, tiled=True),
    )
    return (
        compute_up,
        compute_down,
        compute_norm,
        stepped_up,
        stepped_down,
        stepped_norm,
        state_new_up,
        state_new_down,
        state_new_norm,
    )


def either(*args):
    (R, C), (H, W) = args[3].shape, args[4].shape
    V = args[5].shape[0]
    aligned = R == 128 and W == 128 and V == 128 and C % 128 == 0 and H % 128 == 0
    return fused(*args) if aligned else local(*args)


def solution(mesh):
    return jax.shard_map(
        either,
        mesh=mesh,
        in_specs=(
            P("dp", None, "tp"),
            P("dp", "tp", None),
            P("dp", None),
            P("dp", "tp"),
            P("tp", "dp"),
            P("dp"),
            P("dp", "tp"),
            P("tp", "dp"),
            P("dp"),
        ),
        out_specs=(
            P(None, "tp"),
            P("tp", None),
            P(),
            P("dp", "tp"),
            P("tp", "dp"),
            P("dp"),
            P("dp", "tp"),
            P("tp", "dp"),
            P("dp"),
        ),
        check_vma=False,
    )
```
